32 devices in a mesh: dp: 4 (over y, z), ep: 8 (over x, core).
Axes of the slice: x: 4, y: 2, z: 2, core: 2. Of those that a mesh axis runs over, the one named last changes fastest.
The devices are a block of a 4x4x8 slice.
Arguments:
- x: bfloat16 [96, 128, 2048], P(('dp', 'ep')), parts along dimension 0
- idx: int32 [96, 128, 8], P(('dp', 'ep')), parts along dimension 0
- gates: float32 [96, 128, 8], P(('dp', 'ep')), parts along dimension 0
- g1: float32 [2048], replicated
- wq: bfloat16 [2048, 4096], replicated
- wk: bfloat16 [2048, 4096], replicated
- wv: bfloat16 [2048, 4096], replicated
- wo: bfloat16 [4096, 2048], replicated
- g2: float32 [2048], replicated
- w1: bfloat16 [128, 2048, 768], P('ep')
- w3: bfloat16 [128, 2048, 768], P('ep')
- w2: bfloat16 [128, 768, 2048], P('ep')
Outputs:
- output: bfloat16 [96, 128, 2048], P(('dp', 'ep')), parts along dimension 0
There are 4 independent parts. The reference program is written for one: setup_inputs(seed, part) draws one part's arguments, and reference() takes and returns one part's arrays. A program takes and returns all parts, laid end to end along the dimension named above; an argument that names none is the same for every part.
All inputs are finite; a program needn't handle non-finite values.
Results may differ from the reference program's by a relative error of at most 0.0130551.
Values are sent between devices in bfloat16 or wider.
A program may use at most 768 MiB of HBM per device.

```python
import jax
import jax.numpy as jnp
from jax import lax

D = 2048
HEADS = 32
HEAD = 128
EXPERTS = 128
TOP = 8
FF = 768
SEQ = 128
SEQS = 3
EP = 8

TOK = SEQS * SEQ
AVG = TOP * TOK // EXPERTS
CAP = AVG + AVG // 2
EPS = 1e-6


def draw_routes(kk, shift):
    k1, k2, k3, k4 = jax.random.split(kk, 4)
    signs = jnp.roll(jnp.where(jnp.arange(EXPERTS) < EXPERTS // 2, 1, -1), shift)
    counts = AVG + (AVG // 2) * signs
    ends = jnp.cumsum(counts)
    ent = jnp.searchsorted(ends, jnp.arange(TOP * TOK), side='right').astype(jnp.int32)
    grid = ent.reshape(TOP, TOK).T
    grid = jnp.roll(grid, jax.random.randint(k2, (), 0, TOK), axis=0)
    gates = 2.5 * jax.nn.softmax(0.5 * jax.random.normal(k4, (TOK, TOP), jnp.float32), axis=-1)
    return grid, gates


def setup_inputs(seed: int = 0, part: int = 0) -> dict:
    kp = jax.random.fold_in(jax.random.key(seed), part)
    kx, kr = jax.random.split(kp)
    x = jax.random.normal(kx, (EP * SEQS, SEQ, D), jnp.float32).astype(jnp.bfloat16)
    shift = jax.random.randint(jax.random.fold_in(kr, 7), (), 0, EXPERTS)
    idx, gates = jax.vmap(lambda kk: draw_routes(kk, shift))(jax.random.split(kr, EP))
    ks = jax.random.split(jax.random.key(seed + 1), 9)
    wid = HEADS * HEAD

    def mat(k, shape, scale):
        return (scale * jax.random.normal(k, shape, jnp.float32)).astype(jnp.bfloat16)

    return {
        'x': x,
        'idx': idx.reshape(EP * SEQS, SEQ, TOP),
        'gates': gates.reshape(EP * SEQS, SEQ, TOP),
        'g1': jax.random.uniform(ks[0], (D,), jnp.float32, 0.5, 1.5),
        'wq': mat(ks[1], (D, wid), 1.4 * D ** -0.5),
        'wk': mat(ks[2], (D, wid), 1.4 * D ** -0.5),
        'wv': mat(ks[3], (D, wid), D ** -0.5),
        'wo': mat(ks[4], (wid, D), 2.0 * wid ** -0.5),
        'g2': jax.random.uniform(ks[5], (D,), jnp.float32, 0.5, 1.5),
        'w1': mat(ks[6], (EXPERTS, D, FF), D ** -0.5),
        'w3': mat(ks[7], (EXPERTS, D, FF), D ** -0.5),
        'w2': mat(ks[8], (EXPERTS, FF, D), FF ** -0.5),
    }


def rms(x, g):
    xf = x.astype(jnp.float32)
    return (xf * lax.rsqrt(jnp.mean(xf * xf, axis=-1, keepdims=True) + EPS) * g).astype(jnp.bfloat16)


def attend(q, k, v):
    n = q.shape[0]
    s = jnp.einsum('qhd,khd->hqk', q.astype(jnp.float32), k.astype(jnp.float32)) * HEAD ** -0.5
    mask = jnp.arange(n)[:, None] >= jnp.arange(n)[None, :]
    s = jnp.where(mask[None], s, -1e30)
    p = jax.nn.softmax(s, axis=-1).astype(jnp.bfloat16)
    o = jnp.einsum('hqk,khd->qhd', p.astype(jnp.float32), v.astype(jnp.float32))
    return o.astype(jnp.bfloat16)


def slot_pos(flat):
    n = flat.shape[0]
    order = jnp.argsort(flat, stable=True)
    se = flat[order]
    counts = jnp.zeros((EXPERTS,), jnp.int32).at[flat].add(1)
    starts = jnp.cumsum(counts) - counts
    ps = jnp.arange(n, dtype=jnp.int32) - starts[se]
    return jnp.zeros((n,), jnp.int32).at[order].set(ps)


def expert(a):
    r, a1, a3, a2 = a
    h1 = jnp.dot(r, a1, preferred_element_type=jnp.float32)
    h3 = jnp.dot(r, a3, preferred_element_type=jnp.float32)
    u = (jax.nn.silu(h1) * h3).astype(jnp.bfloat16)
    return jnp.dot(u, a2, preferred_element_type=jnp.float32).astype(jnp.bfloat16)


def reference(x, idx, gates, g1, wq, wk, wv, wo, g2, w1, w3, w2):
    n, s_len, d = x.shape
    t_all = n * s_len
    xf = x.reshape(t_all, d)
    xn = rms(xf, g1)

    def proj(w):
        return jnp.dot(xn, w, preferred_element_type=jnp.float32).astype(jnp.bfloat16).reshape(n, s_len, HEADS, HEAD)

    q = proj(wq)
    k = proj(wk)
    v = proj(wv)
    o = lax.map(lambda a: attend(a[0], a[1], a[2]), (q, k, v))
    att = jnp.dot(o.reshape(t_all, HEADS * HEAD), wo, preferred_element_type=jnp.float32).astype(jnp.bfloat16)
    h = (xf.astype(jnp.float32) + att.astype(jnp.float32)).astype(jnp.bfloat16)
    z = rms(h, g2)
    zs = z.reshape(EP, TOK, d)
    flat = idx.reshape(EP, TOK * TOP)
    dest = flat * CAP + jax.vmap(slot_pos)(flat)
    rows = jnp.repeat(zs, TOP, axis=1)
    buf = jax.vmap(lambda dd, rr: jnp.zeros((EXPERTS * CAP, d), jnp.bfloat16).at[dd].set(rr))(dest, rows)
    buf = buf.reshape(EP, EXPERTS, CAP, d).transpose(1, 0, 2, 3).reshape(EXPERTS, EP * CAP, d)
    out = lax.map(expert, (buf, w1, w3, w2))
    out = out.reshape(EXPERTS, EP, CAP, d).transpose(1, 0, 2, 3).reshape(EP, EXPERTS * CAP, d)
    got = jax.vmap(lambda oo, dd: oo[dd])(out, dest)
    got = got.reshape(t_all, TOP, d).astype(jnp.float32)
    moe = jnp.sum(got * gates.reshape(t_all, TOP, 1), axis=1)
    y = (h.astype(jnp.float32) + moe).astype(jnp.bfloat16)
    return y.reshape(n, s_len, d)
```

```python
import functools

import jax
import jax.numpy as jnp
from jax import lax
from jax.experimental import pallas as pl
from jax.experimental.pallas import tpu as pltpu
from jax.sharding import PartitionSpec as P

EPS = 1e-6
HEAD = 128
MESH = pl.DeviceIdType.MESH
F32 = jnp.float32
BF16 = jnp.bfloat16
VMEM_LIMIT = 67043328
NC = 4
MAIN = 32
OVER = 4
CB = 256


def rms(x, g):
    xf = x.astype(F32)
    return (xf * lax.rsqrt(jnp.mean(xf * xf, axis=-1, keepdims=True) + EPS) * g).astype(BF16)


def dot(a, b):
    return jnp.dot(a, b, preferred_element_type=F32)


def attn_kernel(nseq, x_ref, g1_ref, g2_ref, wq_ref, wk_ref, wv_ref, wo_ref, h_ref, z_ref, xn, o_buf, acc):
    i = pl.program_id(0)
    s_len = x_ref.shape[0] // nseq

    @pl.when(i == 0)
    def _():
        xn[...] = rms(x_ref[...], g1_ref[...])
        acc[...] = jnp.zeros_like(acc)

    a = xn[...]
    q = dot(a, wq_ref[...]).astype(BF16)
    k = dot(a, wk_ref[...]).astype(BF16)
    v = dot(a, wv_ref[...]).astype(BF16)
    row = lax.broadcasted_iota(jnp.int32, (s_len, s_len), 0)
    col = lax.broadcasted_iota(jnp.int32, (s_len, s_len), 1)
    mask = row >= col
    for s in range(nseq):
        for hd in range(wq_ref.shape[1] // HEAD):
            r = slice(s * s_len, (s + 1) * s_len)
            c = slice(hd * HEAD, (hd + 1) * HEAD)
            sc = lax.dot_general(q[r, c], k[r, c], (((1,), (1,)), ((), ())), preferred_element_type=F32) * HEAD ** -0.5
            sc = jnp.where(mask, sc, -1e30)
            e = jnp.exp(sc - jnp.max(sc, axis=-1, keepdims=True))
            p = (e / jnp.sum(e, axis=-1, keepdims=True)).astype(BF16)
            o_buf[r, c] = dot(p, v[r, c]).astype(BF16)
    acc[...] += dot(o_buf[...], wo_ref[...])

    @pl.when(i == pl.num_programs(0) - 1)
    def _():
        h = (x_ref[...].astype(F32) + acc[...].astype(BF16).astype(F32)).astype(BF16)
        h_ref[...] = h
        z = rms(h, g2_ref[...])
        w = z_ref.shape[2]
        for c in range(z_ref.shape[0]):
            z_ref[c] = z[:, c * w:(c + 1) * w]


def attention(xf, g1, g2, wq, wk, wv, wo, nseq):
    t, d = xf.shape
    wid = wq.shape[1]
    hb = 256
    full = pl.BlockSpec((t, d), lambda i: (0, 0))
    vec = pl.BlockSpec((1, d), lambda i: (0, 0))
    wspec = pl.BlockSpec((d, hb), lambda i: (0, i))
    return pl.pallas_call(
        functools.partial(attn_kernel, nseq),
        grid=(wid // hb,),
        in_specs=[full, vec, vec, wspec, wspec, wspec, pl.BlockSpec((hb, d), lambda i: (i, 0))],
        out_specs=[full, pl.BlockSpec((NC, t, d // NC), lambda i: (0, 0, 0))],
        out_shape=[jax.ShapeDtypeStruct((t, d), BF16), jax.ShapeDtypeStruct((NC, t, d // NC), BF16)],
        scratch_shapes=[pltpu.VMEM((t, d), BF16), pltpu.VMEM((t, hb), BF16), pltpu.VMEM((t, d), F32)],
        compiler_params=pltpu.CompilerParams(vmem_limit_bytes=VMEM_LIMIT),
        name="attention",
    )(xf, g1.reshape(1, d), g2.reshape(1, d), wq, wk, wv, wo)


def local_ranks(meta, base, n_loc):
    top, t = meta.shape[0] // 2, meta.shape[1]
    e = lax.broadcasted_iota(jnp.int32, (n_loc, t), 0).astype(F32) + base
    m = jnp.zeros((n_loc, t), F32)
    g = jnp.zeros((n_loc, t), F32)
    for j in range(top):
        hit = meta[j:j + 1, :] == e
        m = m + jnp.where(hit, 1.0, 0.0)
        g = g + jnp.where(hit, meta[top + j:top + j + 1, :], 0.0)
    before = lax.broadcasted_iota(jnp.int32, (t, t), 0) < lax.broadcasted_iota(jnp.int32, (t, t), 1)
    rank = dot(m.astype(BF16), jnp.where(before, 1.0, 0.0).astype(BF16))
    return jnp.where(m > 0.5, rank, 255.0).astype(BF16), g


def slot_of(q, src, n_loc):
    main = n_loc * MAIN
    is_main = q < main
    qo = q - main
    ko = qo % (4 * OVER)
    exp = jnp.where(is_main, q // MAIN, qo // (4 * OVER))
    rank = jnp.where(is_main, q % MAIN, jnp.where(ko // OVER == src % 4, MAIN + ko % OVER, -1))
    return exp, rank


def up_kernel(n_loc, z_ref, meta_ref, w1_ref, w3_ref, u_ref, gm_ref,
              zr, ss, xbuf, acc, wbuf, ubuf, zsem, wsem, usem, m_send, m_recv, ssem, rsem):
    ep = lax.axis_size("ep")
    me = lax.axis_index("ep")
    core = lax.rem(me, 2)
    chip = lax.div(me, 2)
    nch = ep // 2
    other = me + 1 - 2 * core

    def dev(ch, co):
        return 2 * lax.rem(ch + nch, nch) + co

    right, left, far = dev(chip + 1, core), dev(chip - 1, core), dev(chip + 2, core)
    orig, olef, ofar, own_o = dev(chip + 1, 1 - core), dev(chip - 1, 1 - core), dev(chip + 2, 1 - core), other
    t, ck = zr.shape[2], zr.shape[3]
    half = t // 2
    ff = w1_ref.shape[2]
    W = wbuf.shape[0]

    def zload(k):
        return pltpu.make_async_copy(z_ref.at[k], zr.at[k, me], zsem.at[k])

    for k in range(NC):
        zload(k).start()

    def wload(i):
        slot = lax.rem(i, W)
        e = lax.rem(i, n_loc)
        k0 = pl.multiple_of(lax.div(i, n_loc) * ck, ck)
        return (pltpu.make_async_copy(w1_ref.at[e, pl.ds(k0, ck), :], wbuf.at[slot, 0], wsem.at[slot, 0]),
                pltpu.make_async_copy(w3_ref.at[e, pl.ds(k0, ck), :], wbuf.at[slot, 1], wsem.at[slot, 1]))

    for i in range(W - 1):
        for c in wload(i):
            c.start()

    barrier = pltpu.get_barrier_semaphore()
    for off in range(1, 8):
        pl.semaphore_signal(barrier, inc=1, device_id={"ep": lax.rem(me + off, ep)}, device_id_type=MESH)
    pl.semaphore_wait(barrier, 7)

    def mcopy(off, slot):
        return pltpu.make_async_remote_copy(meta_ref, gm_ref.at[slot], m_send.at[off - 1], m_recv.at[off - 1],
                                            device_id={"ep": lax.rem(me + off, ep)}, device_id_type=MESH)

    for off in range(1, 8):
        mcopy(off, me).start()

    lo, hi, al = pl.ds(0, half), pl.ds(half, half), pl.ds(0, t)

    def rc(kind, k, src, rows, to):
        ref = zr.at[k, src, rows]
        return pltpu.make_async_remote_copy(ref, ref, ssem.at[kind, k], rsem.at[kind, k],
                                            device_id={"ep": to}, device_id_type=MESH)

    def sends(k):
        return {
            0: rc(0, k, me, lo, right), 1: rc(1, k, me, hi, right),
            2: rc(2, k, me, hi, left), 3: rc(3, k, me, lo, left),
            4: rc(4, k, left, lo, right), 5: rc(5, k, right, hi, left),
            6: rc(6, k, me, al, other), 7: rc(7, k, left, al, other), 8: rc(8, k, right, al, other),
            9: rc(9, k, far, lo, other), 10: rc(10, k, far, hi, other),
        }

    def recvs(k):
        return {
            0: rc(0, k, left, lo, right), 1: rc(1, k, left, hi, right),
            2: rc(2, k, right, hi, left), 3: rc(3, k, right, lo, left),
            4: rc(4, k, far, lo, right), 5: rc(5, k, far, hi, left),
            6: rc(6, k, own_o, al, other), 7: rc(7, k, olef, al, other), 8: rc(8, k, orig, al, other),
            9: rc(9, k, ofar, lo, other), 10: rc(10, k, ofar, hi, other),
        }

    S = [sends(k) for k in range(NC)]
    R = [recvs(k) for k in range(NC)]

    def own(k):
        zload(k).wait()
        for kind in (0, 2, 1, 3, 6):
            S[k][kind].start()

    def poll_a(k):
        R[k][0].wait_recv()
        S[k][4].start()
        R[k][2].wait_recv()
        S[k][5].start()
        if k + 1 < NC:
            own(k + 1)

    def poll_b(k):
        R[k][1].wait_recv()
        S[k][7].start()
        R[k][3].wait_recv()
        S[k][8].start()

    def poll_c(k):
        R[k][4].wait_recv()
        S[k][9].start()
        R[k][5].wait_recv()
        S[k][10].start()
        for kind in (6, 7, 8, 9, 10):
            R[k][kind].wait_recv()

    own(0)
    gm_ref[me] = meta_ref[...]
    for off in range(1, 8):
        mcopy(off, lax.rem(me - off + ep, ep)).wait_recv()
    base = (me * n_loc).astype(F32)

    rows = ss.shape[1]

    def build(s, _):
        rank, _g = local_ranks(gm_ref[s], base, n_loc)
        q1 = lax.broadcasted_iota(jnp.int32, (rows, n_loc), 0)
        e1 = lax.broadcasted_iota(jnp.int32, (rows, n_loc), 1)
        ex = jnp.where(slot_of(q1, s, n_loc)[0] == e1, 1.0, 0.0).astype(BF16)
        r = dot(ex, rank)
        want = slot_of(lax.broadcasted_iota(jnp.int32, (rows, t), 0), s, n_loc)[1].astype(F32)
        ss[s] = jnp.where(r == want, 1.0, 0.0).astype(BF16)
        return 0

    lax.fori_loop(0, 4, build, 0)
    poll_a(0)
    lax.fori_loop(4, 8, build, 0)
    poll_b(0)
    poll_c(0)

    main = n_loc * MAIN

    def expert(k, e, _):
        i = k * n_loc + e
        slot = lax.rem(i, W)

        @pl.when(i + W - 1 < NC * n_loc)
        def _():
            for c in wload(i + W - 1):
                c.start()

        for c in wload(i):
            c.wait()
        x = xbuf[e]
        h1 = dot(x, wbuf[slot, 0])
        h3 = dot(x, wbuf[slot, 1])
        if k == 0:
            acc[e, 0] = h1
            acc[e, 1] = h3
        elif k < NC - 1:
            acc[e, 0] += h1
            acc[e, 1] += h3
        else:
            us = lax.rem(e, 2)

            @pl.when(e >= 2)
            def _():
                pltpu.make_async_copy(ubuf.at[us], u_ref.at[e - 2], usem.at[us]).wait()

            h1 = acc[e, 0] + h1
            h3 = acc[e, 1] + h3
            ubuf[us] = (h1 * jax.nn.sigmoid(h1) * h3).astype(BF16)
            pltpu.make_async_copy(ubuf.at[us], u_ref.at[e], usem.at[us]).start()
        return 0

    for k in range(NC):
        for hf in range(2):
            over = None
            for s4 in range(4):
                s = 4 * hf + s4
                g = dot(ss[s], zr[k, s])
                xbuf[:, s * MAIN:(s + 1) * MAIN, :] = g[:main].astype(BF16).reshape(n_loc, MAIN, ck)
                over = g[main:] if over is None else over + g[main:]
            o0 = 8 * MAIN + hf * 4 * OVER
            xbuf[:, o0:o0 + 4 * OVER, :] = over.astype(BF16).reshape(n_loc, 4 * OVER, ck)
        body = functools.partial(expert, k)
        if k + 1 < NC:
            lax.fori_loop(0, 4, body, 0)
            poll_a(k + 1)
            lax.fori_loop(4, 10, body, 0)
            poll_b(k + 1)
            lax.fori_loop(10, n_loc, body, 0)
            poll_c(k + 1)
        else:
            lax.fori_loop(0, n_loc, body, 0)

    for e in (n_loc - 2, n_loc - 1):
        pltpu.make_async_copy(ubuf.at[e % 2], u_ref.at[e], usem.at[e % 2]).wait()
    for off in range(1, 8):
        mcopy(off, me).wait_send()
    for k in range(NC):
        for kind in range(11):
            S[k][kind].wait_send()


def gather_up(z, meta, w1, w3):
    n_loc, d, ff = w1.shape
    nc, t, ck = z.shape
    rows = n_loc * (MAIN + 4 * OVER)
    per = 8 * MAIN + 8 * OVER
    wslots = 4
    anys = pl.BlockSpec(memory_space=pl.ANY)
    vm = pl.BlockSpec(memory_space=pltpu.VMEM)
    return pl.pallas_call(
        functools.partial(up_kernel, n_loc),
        in_specs=[anys, vm, anys, anys],
        out_specs=[anys, vm],
        out_shape=[jax.ShapeDtypeStruct((n_loc, per, ff), BF16), jax.ShapeDtypeStruct((8,) + meta.shape, F32)],
        scratch_shapes=[
            pltpu.VMEM((nc, 8, t, ck), BF16),
            pltpu.VMEM((8, rows, t), BF16),
            pltpu.VMEM((n_loc, per, ck), BF16),
            pltpu.VMEM((n_loc, 2, per, ff), F32),
            pltpu.VMEM((wslots, 2, ck, ff), BF16),
            pltpu.VMEM((2, per, ff), BF16),
            pltpu.SemaphoreType.DMA((nc,)),
            pltpu.SemaphoreType.DMA((wslots, 2)),
            pltpu.SemaphoreType.DMA((2,)),
            pltpu.SemaphoreType.DMA((7,)),
            pltpu.SemaphoreType.DMA((7,)),
            pltpu.SemaphoreType.DMA((11, nc)),
            pltpu.SemaphoreType.DMA((11, nc)),
        ],
        compiler_params=pltpu.CompilerParams(vmem_limit_bytes=VMEM_LIMIT, collective_id=0, has_side_effects=True),
        name="gather_up",
    )(z, meta, w1, w3)


def down_kernel(n_loc, u_ref, gm_ref, w2_ref, h_ref, y_ref,
                ub, gg, ecat, wbuf, pbuf, qbuf, tbuf, drecv, xrecv, usem, wsem, dss, drs, xss, xrs):
    ep = lax.axis_size("ep")
    me = lax.axis_index("ep")
    core = lax.rem(me, 2)
    chip = lax.div(me, 2)
    nch = ep // 2
    other = me + 1 - 2 * core
    t = h_ref.shape[0]
    ncb = h_ref.shape[1] // CB
    W = wbuf.shape[0]
    main = n_loc * MAIN
    rows = n_loc * (MAIN + 4 * OVER)
    hc = CB // 2

    def dev(ch, co):
        return 2 * lax.rem(ch + nch, nch) + co

    right, left = dev(chip + 1, core), dev(chip - 1, core)

    ucopy = pltpu.make_async_copy(u_ref, ub, usem)
    ucopy.start()

    def wload(i):
        slot = lax.rem(i, W)
        e = lax.rem(i, n_loc)
        c0 = pl.multiple_of(lax.div(i, n_loc) * CB, CB)
        return pltpu.make_async_copy(w2_ref.at[e, :, pl.ds(c0, CB)], wbuf.at[slot], wsem.at[slot])

    for i in range(W - 1):
        wload(i).start()

    barrier = pltpu.get_barrier_semaphore()
    for peer in (right, left, other):
        pl.semaphore_signal(barrier, inc=1, device_id={"ep": peer}, device_id_type=MESH)
    pl.semaphore_wait(barrier, 3)

    base = (me * n_loc).astype(F32)

    def build(s, _):
        rank, g = local_ranks(gm_ref[s], base, n_loc)
        g_hi = g.astype(BF16)
        r1 = g - g_hi.astype(F32)
        g_mid = r1.astype(BF16)
        g_lo = (r1 - g_mid.astype(F32)).astype(BF16)
        e1 = lax.broadcasted_iota(jnp.int32, (n_loc, rows), 0)
        q1 = lax.broadcasted_iota(jnp.int32, (n_loc, rows), 1)
        ex = jnp.where(slot_of(q1, s, n_loc)[0] == e1, 1.0, 0.0).astype(BF16)
        want = slot_of(lax.broadcasted_iota(jnp.int32, (t, rows), 1), s, n_loc)[1].astype(F32)

        def expand(a):
            return lax.dot_general(a, ex, (((0,), (0,)), ((), ())), preferred_element_type=F32)

        keep = expand(rank) == want
        for n, part in enumerate((g_hi, g_mid, g_lo)):
            gg[s, :, n * rows:(n + 1) * rows] = jnp.where(keep, expand(part), 0.0).astype(BF16)
        return 0

    lax.fori_loop(0, 8, build, 0)
    ucopy.wait()

    def partial(s):
        e = ecat[s]
        return (dot(gg[s, :, 0:rows], e) + dot(gg[s, :, rows:2 * rows], e)) + dot(gg[s, :, 2 * rows:3 * rows], e)

    def dst(j):
        return lax.rem(chip + jnp.where(j == 0, 2, jnp.where(j == 1, 1, jnp.where(j == 2, 3, 0))), nch)

    def dcopy(n, j):
        sl = lax.rem(n, 2)
        return pltpu.make_async_remote_copy(pbuf.at[sl, j], drecv.at[n, j], dss.at[sl, j], drs.at[n, j],
                                            device_id={"ep": other}, device_id_type=MESH)

    def xcopy(n, kind):
        sl = lax.rem(n, 3)
        src = {0: qbuf.at[sl, 0, 0], 1: qbuf.at[sl, 0, 1], 2: qbuf.at[sl, 1, 0], 3: qbuf.at[sl, 2, 1],
               4: tbuf.at[lax.rem(n, 2), 0], 5: tbuf.at[lax.rem(n, 2), 1]}[kind]
        to = left if kind in (0, 3, 4) else right
        ssl = sl if kind < 4 else lax.rem(n, 2)
        return pltpu.make_async_remote_copy(src, xrecv.at[n, kind], xss.at[kind, ssl], xrs.at[n, kind],
                                            device_id={"ep": to}, device_id_type=MESH)

    def stage_a(n):
        sl = lax.rem(n, 2)
        sq = lax.rem(n, 3)

        def expert(e, _):
            i = n * n_loc + e

            @pl.when(i + W - 1 < ncb * n_loc)
            def _():
                wload(i + W - 1).start()

            wload(i).wait()
            o = dot(ub[e], wbuf[lax.rem(i, W)]).astype(BF16)
            r0 = pl.multiple_of(e * MAIN, MAIN)
            r1 = pl.multiple_of(main + e * 4 * OVER, 4 * OVER)
            for s in range(8):
                ecat[s, pl.ds(r0, MAIN), :] = o[s * MAIN:(s + 1) * MAIN]
                b = 8 * MAIN + (s // 4) * 4 * OVER
                ecat[s, pl.ds(r1, 4 * OVER), :] = o[b:b + 4 * OVER]
            return 0

        lax.fori_loop(0, n_loc, expert, 0)

        def theirs(j, _):
            @pl.when(n >= 2)
            def _():
                dcopy(n - 2, j).wait_send()

            pbuf[sl, j] = partial(2 * dst(j) + 1 - core)
            dcopy(n, j).start()
            return 0

        lax.fori_loop(0, 4, theirs, 0)

        @pl.when(n >= 3)
        def _():
            for kind in range(4):
                xcopy(n - 3, kind).wait_send()

        def ours(j, _):
            p = partial(2 * dst(j) + core)
            dcopy(n, j).wait_recv()
            p = p + drecv[n, j]
            qbuf[sq, j, 0] = p[:, :hc]
            qbuf[sq, j, 1] = p[:, hc:]

            @pl.when(j == 0)
            def _():
                xcopy(n, 0).start()
                xcopy(n, 1).start()

            @pl.when(j == 1)
            def _():
                xcopy(n, 2).start()

            @pl.when(j == 2)
            def _():
                xcopy(n, 3).start()

            return 0

        lax.fori_loop(0, 4, ours, 0)

    def stage_c(n):
        sq = lax.rem(n, 3)
        st = lax.rem(n, 2)

        @pl.when(n >= 2)
        def _():
            xcopy(n - 2, 4).wait_send()
            xcopy(n - 2, 5).wait_send()

        xcopy(n, 0).wait_recv()
        tbuf[st, 0] = qbuf[sq, 2, 0] + xrecv[n, 0]
        xcopy(n, 4).start()
        xcopy(n, 1).wait_recv()
        tbuf[st, 1] = qbuf[sq, 1, 1] + xrecv[n, 1]
        xcopy(n, 5).start()

    def stage_d(n):
        sq = lax.rem(n, 3)
        for kind in (2, 3, 4, 5):
            xcopy(n, kind).wait_recv()
        c0 = pl.multiple_of(n * CB, CB)
        a = (qbuf[sq, 3, 0] + xrecv[n, 2]) + xrecv[n, 4]
        b = (qbuf[sq, 3, 1] + xrecv[n, 3]) + xrecv[n, 5]
        y_ref[:, pl.ds(c0, hc)] = (h_ref[:, pl.ds(c0, hc)].astype(F32) + a).astype(BF16)
        y_ref[:, pl.ds(c0 + hc, hc)] = (h_ref[:, pl.ds(c0 + hc, hc)].astype(F32) + b).astype(BF16)

    def step(n, _):
        @pl.when(n < ncb)
        def _():
            stage_a(n)

        @pl.when(jnp.logical_and(n >= 1, n - 1 < ncb))
        def _():
            stage_c(n - 1)

        @pl.when(n >= 2)
        def _():
            stage_d(n - 2)

        return 0

    lax.fori_loop(0, ncb + 2, step, 0)

    for n in (ncb - 2, ncb - 1):
        for j in range(4):
            dcopy(n, j).wait_send()
        for kind in (4, 5):
            xcopy(n, kind).wait_send()
    for n in (ncb - 3, ncb - 2, ncb - 1):
        for kind in range(4):
            xcopy(n, kind).wait_send()


def down_reduce(u, gm, w2, h):
    n_loc, ff, d = w2.shape
    t = h.shape[0]
    ncb = d // CB
    rows = n_loc * (MAIN + 4 * OVER)
    wslots = 6
    anys = pl.BlockSpec(memory_space=pl.ANY)
    vm = pl.BlockSpec(memory_space=pltpu.VMEM)
    return pl.pallas_call(
        functools.partial(down_kernel, n_loc),
        in_specs=[anys, vm, anys, vm],
        out_specs=vm,
        out_shape=jax.ShapeDtypeStruct((t, d), BF16),
        scratch_shapes=[
            pltpu.VMEM(u.shape, BF16),
            pltpu.VMEM((8, t, 3 * rows), BF16),
            pltpu.VMEM((8, rows, CB), BF16),
            pltpu.VMEM((wslots, ff, CB), BF16),
            pltpu.VMEM((2, 4, t, CB), F32),
            pltpu.VMEM((3, 4, 2, t, CB // 2), F32),
            pltpu.VMEM((2, 2, t, CB // 2), F32),
            pltpu.VMEM((ncb, 4, t, CB), F32),
            pltpu.VMEM((ncb, 6, t, CB // 2), F32),
            pltpu.SemaphoreType.DMA,
            pltpu.SemaphoreType.DMA((wslots,)),
            pltpu.SemaphoreType.DMA((2, 4)),
            pltpu.SemaphoreType.DMA((ncb, 4)),
            pltpu.SemaphoreType.DMA((6, 3)),
            pltpu.SemaphoreType.DMA((ncb, 6)),
        ],
        compiler_params=pltpu.CompilerParams(vmem_limit_bytes=VMEM_LIMIT, collective_id=1, has_side_effects=True),
        name="down_reduce",
    )(u, gm, w2, h)


def solution(mesh):
    tok = P(('dp', 'ep'))
    rep = P()
    exs = P('ep')

    def body(x, idx, gates, g1, wq, wk, wv, wo, g2, w1, w3, w2):
        n, s_len, d = x.shape
        t = n * s_len
        top = idx.shape[-1]
        meta = jnp.concatenate([idx.reshape(t, top).T.astype(F32), gates.reshape(t, top).T], axis=0)
        h, z = attention(x.reshape(t, d), g1, g2, wq, wk, wv, wo, n)
        u, gm = gather_up(z, meta, w1, w3)
        y = down_reduce(u, gm, w2, h)
        return y.reshape(n, s_len, d)

    return jax.shard_map(body, mesh=mesh, in_specs=(tok, tok, tok, rep, rep, rep, rep, rep, rep, exs, exs, exs), out_specs=tok, check_vma=False)
```

```python
import functools

import jax
import jax.numpy as jnp
from jax import lax
from jax.experimental import pallas as pl
from jax.experimental.pallas import tpu as pltpu
from jax.sharding import PartitionSpec as P

EPS = 1e-6
HEAD = 128
MESH = pl.DeviceIdType.MESH
F32 = jnp.float32
BF16 = jnp.bfloat16
VMEM_LIMIT = 67043328
HB = 512
CHUNKS = (256, 512, 512, 512, 256)
KB = 256
MAIN = 32
OVER = 4
CB = 256


def rms(x, g):
    xf = x.astype(F32)
    return (xf * lax.rsqrt(jnp.mean(xf * xf, axis=-1, keepdims=True) + EPS) * g).astype(BF16)


def dot(a, b):
    return jnp.dot(a, b, preferred_element_type=F32)


def attn_kernel(nseq, x_ref, idx_ref, gates_ref, g1_ref, g2_ref, wq_ref, wk_ref, wv_ref, wo_ref, h_ref, z_ref, meta_ref, xn, qkv, o_buf, s_buf, p_buf, acc):
    i = pl.program_id(0)
    s_len = x_ref.shape[0] // nseq
    blocks = x_ref.shape[0] // 32

    @pl.when(i == 0)
    def _():
        def ini(b, _):
            r = pl.ds(pl.multiple_of(b * 32, 32), 32)
            xn[r, :] = rms(x_ref[r, :], g1_ref[...])
            acc[r, :] = jnp.zeros((32, acc.shape[1]), F32)
            return 0
        lax.fori_loop(0, blocks, ini, 0)
        top = idx_ref.shape[1]
        for s in range(nseq):
            c = slice(s * s_len, (s + 1) * s_len)
            meta_ref[:top, c] = idx_ref[s].astype(F32)
            meta_ref[top:, c] = gates_ref[s]

    row = lax.broadcasted_iota(jnp.int32, (s_len, s_len), 0)
    col = lax.broadcasted_iota(jnp.int32, (s_len, s_len), 1)
    mask = row >= col
    heads = wq_ref.shape[1] // HEAD
    pairs = [(s * heads + hd, slice(s * s_len, (s + 1) * s_len), slice(hd * HEAD, (hd + 1) * HEAD))
             for s in range(nseq) for hd in range(heads)]

    qkv[0] = dot(xn[...], wq_ref[...]).astype(BF16)
    qkv[1] = dot(xn[...], wk_ref[...]).astype(BF16)
    for n, r, c in pairs:
        sc = lax.dot_general(qkv[0, r, c], qkv[1, r, c], (((1,), (1,)), ((), ())), preferred_element_type=F32)
        s_buf[n] = jnp.where(mask, sc * HEAD ** -0.5, -1e30)
    for n, r, c in pairs:
        sc = s_buf[n]
        e = jnp.exp(sc - jnp.max(sc, axis=-1, keepdims=True))
        p_buf[n] = (e * (1.0 / jnp.sum(e, axis=-1, keepdims=True))).astype(BF16)
    qkv[2] = dot(xn[...], wv_ref[...]).astype(BF16)
    for n, r, c in pairs:
        o_buf[r, c] = dot(p_buf[n], qkv[2, r, c]).astype(BF16)
    acc[...] += dot(o_buf[...], wo_ref[...])

    @pl.when(i == pl.num_programs(0) - 1)
    def _():
        def fin(b, _):
            r = pl.ds(pl.multiple_of(b * 32, 32), 32)
            h = (x_ref[r, :].astype(F32) + acc[r, :].astype(BF16).astype(F32)).astype(BF16)
            h_ref[r, :] = h
            z_ref[r, :] = rms(h, g2_ref[...])
            return 0
        lax.fori_loop(0, blocks, fin, 0)


def attention(xf, idx, gates, g1, g2, wq, wk, wv, wo, nseq):
    t, d = xf.shape
    top = idx.shape[1]
    route = pl.BlockSpec(idx.shape, lambda i: (0, 0, 0))
    wid = wq.shape[1]
    n_pair = nseq * (HB // HEAD)
    s_len = t // nseq
    full = pl.BlockSpec((t, d), lambda i: (0, 0))
    vec = pl.BlockSpec((1, d), lambda i: (0, 0))
    wspec = pl.BlockSpec((d, HB), lambda i: (0, i))
    return pl.pallas_call(
        functools.partial(attn_kernel, nseq),
        grid=(wid // HB,),
        in_specs=[full, route, route, vec, vec, wspec, wspec, wspec, pl.BlockSpec((HB, d), lambda i: (i, 0))],
        out_specs=[full, full, pl.BlockSpec((2 * top, t), lambda i: (0, 0))],
        out_shape=[jax.ShapeDtypeStruct((t, d), BF16), jax.ShapeDtypeStruct((t, d), BF16), jax.ShapeDtypeStruct((2 * top, t), F32)],
        scratch_shapes=[pltpu.VMEM((t, d), BF16), pltpu.VMEM((3, t, HB), BF16), pltpu.VMEM((t, HB), BF16),
                        pltpu.VMEM((n_pair, s_len, s_len), F32), pltpu.VMEM((n_pair, s_len, s_len), BF16), pltpu.VMEM((t, d), F32)],
        compiler_params=pltpu.CompilerParams(vmem_limit_bytes=VMEM_LIMIT),
        name="attention",
    )(xf, idx, gates, g1.reshape(1, d), g2.reshape(1, d), wq, wk, wv, wo)


class Group:
    def __init__(self):
        self.ep = lax.axis_size("ep")
        self.me = lax.axis_index("ep")
        self.core = lax.rem(self.me, 2)
        self.chip = lax.div(self.me, 2)
        self.nch = self.ep // 2
        self.right, self.left, self.far = self.dev(1, 0), self.dev(self.nch - 1, 0), self.dev(2, 0)
        self.other = self.dev(0, 1)
        self.rel = (0, 1, self.nch - 1, 2)

    def dev(self, hop, swap):
        return 2 * lax.rem(self.chip + hop, self.nch) + (1 - self.core if swap else self.core)

    def place(self, p):
        return self.dev(self.rel[p // 2], p % 2)


def local_ranks(meta, base, n_loc):
    top, t = meta.shape[0] // 2, meta.shape[1]
    e = lax.broadcasted_iota(jnp.int32, (n_loc, t), 0).astype(F32) + base
    m = jnp.zeros((n_loc, t), F32)
    g = jnp.zeros((n_loc, t), F32)
    for j in range(top):
        hit = meta[j:j + 1, :] == e
        m = m + jnp.where(hit, 1.0, 0.0)
        g = g + jnp.where(hit, meta[top + j:top + j + 1, :], 0.0)
    before = lax.broadcasted_iota(jnp.int32, (t, t), 0) < lax.broadcasted_iota(jnp.int32, (t, t), 1)
    rank = dot(m.astype(BF16), jnp.where(before, 1.0, 0.0).astype(BF16))
    return jnp.where(m > 0.5, rank, 255.0).astype(BF16), g


def slot_of(q, place, n_loc):
    main = n_loc * MAIN
    is_main = q < main
    qo = q - main
    ko = qo % (4 * OVER)
    exp = jnp.where(is_main, q // MAIN, qo // (4 * OVER))
    rank = jnp.where(is_main, q % MAIN, jnp.where(ko // OVER == place % 4, MAIN + ko % OVER, -1))
    return exp, rank


def up_kernel(n_loc, z_ref, meta_ref, w1_ref, w3_ref, u_ref, gm_ref,
              zr, ss, xbuf, acc, wbuf, ubuf, zsem, wsem, usem, m_send, m_recv, ssem, rsem):
    g = Group()
    me, ep = g.me, g.ep
    t, d = z_ref.shape
    half = t // 2
    ff = w1_ref.shape[2]
    W = wbuf.shape[0]
    nk = len(CHUNKS)
    off = [sum(CHUNKS[:k]) for k in range(nk)]
    rows = ss.shape[1]
    main = n_loc * MAIN
    big_it = n_loc // 2
    small_it = n_loc // 4
    t_first = small_it
    t_last = t_first + (nk - 2) * big_it
    t_all = t_last + small_it

    def zload(k):
        c = pl.ds(off[k], CHUNKS[k])
        return pltpu.make_async_copy(z_ref.at[:, c], zr.at[me, :, c], zsem.at[k])

    for k in range(nk):
        zload(k).start()

    def wload(it, j):
        slot = lax.rem(4 * it + j, W)
        big = jnp.logical_and(it >= t_first, it < t_last)
        bi = it - t_first
        e = jnp.where(big, 2 * lax.rem(bi, big_it) + j // 2, 4 * jnp.where(it < t_first, it, it - t_last) + j)
        r0 = jnp.where(big, KB + lax.div(bi, big_it) * (2 * KB) + (j % 2) * KB, jnp.where(it < t_first, 0, off[-1]))
        r = pl.ds(pl.multiple_of(r0, KB), KB)
        return (pltpu.make_async_copy(w1_ref.at[e, r, :], wbuf.at[slot, 0], wsem.at[slot, 0]),
                pltpu.make_async_copy(w3_ref.at[e, r, :], wbuf.at[slot, 1], wsem.at[slot, 1]))

    ahead = W // 4 - 1
    for i in range(ahead):
        for j in range(4):
            for c in wload(i, j):
                c.start()

    barrier = pltpu.get_barrier_semaphore()
    for o in range(1, 8):
        pl.semaphore_signal(barrier, inc=1, device_id={"ep": lax.rem(me + o, ep)}, device_id_type=MESH)
    pl.semaphore_wait(barrier, 7)

    def mcopy(o, slot):
        return pltpu.make_async_remote_copy(meta_ref, gm_ref.at[slot], m_send.at[o - 1], m_recv.at[o - 1],
                                            device_id={"ep": lax.rem(me + o, ep)}, device_id_type=MESH)

    for o in range(1, 8):
        mcopy(o, me).start()

    lo, hi, al = pl.ds(0, half), pl.ds(half, half), pl.ds(0, t)

    def rc(kind, k, src, part, to):
        ref = zr.at[src, part, pl.ds(off[k], CHUNKS[k])]
        return pltpu.make_async_remote_copy(ref, ref, ssem.at[kind, k], rsem.at[kind, k],
                                            device_id={"ep": to}, device_id_type=MESH)

    ways = (g.right, g.right, g.left, g.left, g.right, g.left) + (g.other,) * 5
    parts = (lo, hi, hi, lo, lo, hi, al, al, al, lo, hi)
    sent = (me,) * 4 + (g.left, g.right, me, g.left, g.right, g.far, g.far)
    got = ((g.left,) * 2 + (g.right,) * 2 + (g.far,) * 2
           + (g.other, g.dev(g.nch - 1, True), g.dev(1, True), g.dev(2, True), g.dev(2, True)))
    KINDS = len(ways)

    def send(kind, k):
        return rc(kind, k, sent[kind], parts[kind], ways[kind])

    def recv(kind, k):
        return rc(kind, k, got[kind], parts[kind], ways[kind])

    def own(k):
        zload(k).wait()
        for kind in (0, 2, 1, 3, 6):
            send(kind, k).start()

    def poll_a(k):
        recv(0, k).wait_recv()
        send(4, k).start()
        recv(2, k).wait_recv()
        send(5, k).start()

    def poll_b(k):
        recv(1, k).wait_recv()
        send(7, k).start()
        recv(3, k).wait_recv()
        send(8, k).start()

    def poll_c(k):
        recv(4, k).wait_recv()
        send(9, k).start()
        recv(5, k).wait_recv()
        send(10, k).start()

    own(0)
    gm_ref[me] = meta_ref[...]
    for o in range(1, 8):
        mcopy(o, lax.rem(me - o + ep, ep)).wait_recv()
    base = (me * n_loc).astype(F32)

    def build(p):
        rank, _g = local_ranks(gm_ref[g.place(p)], base, n_loc)
        for r0 in range(0, rows, 256):
            q1 = lax.broadcasted_iota(jnp.int32, (256, n_loc), 0) + r0
            e1 = lax.broadcasted_iota(jnp.int32, (256, n_loc), 1)
            ex = jnp.where(slot_of(q1, p, n_loc)[0] == e1, 1.0, 0.0).astype(BF16)
            want = slot_of(lax.broadcasted_iota(jnp.int32, (256, t), 0) + r0, p, n_loc)[1].astype(F32)
            ss[p, r0:r0 + 256, :] = jnp.where(dot(ex, rank) == want, 1.0, 0.0).astype(BF16)

    for p in range(4):
        build(p)
    poll_a(0)
    own(1)
    for p in range(4, 8):
        build(p)

    poll_b(0)
    poll_c(0)

    def take(k, p, over):
        ck = CHUNKS[k]
        y = dot(ss[p], zr[g.place(p), :, off[k]:off[k] + ck])
        xbuf[:, p * MAIN:(p + 1) * MAIN, :ck] = y[:main].astype(BF16).reshape(n_loc, MAIN, ck)
        over = y[main:] if p % 4 == 0 else over + y[main:]
        if p % 4 == 3:
            o0 = 8 * MAIN + (p // 4) * 4 * OVER
            xbuf[:, o0:o0 + 4 * OVER, :ck] = over.astype(BF16).reshape(n_loc, 4 * OVER, ck)
        return over

    def gather(k):
        over = None
        for kind in (6, 7, 8):
            recv(kind, k).wait_recv()
        for p in range(6):
            over = take(k, p, over)
        for kind in (9, 10):
            recv(kind, k).wait_recv()
        for p in range(6, 8):
            over = take(k, p, over)

    def ucopy(e):
        us = lax.rem(e, 4)
        return pltpu.make_async_copy(ubuf.at[us], u_ref.at[e], usem.at[us])

    def experts(k, i, _):
        last = k == nk - 1
        big = CHUNKS[k] == 2 * KB
        it = i + (0 if k == 0 else t_last if last else t_first + (k - 1) * big_it)

        @pl.when(it + ahead < t_all)
        def _():
            for j in range(4):
                for c in wload(it + ahead, j):
                    c.start()

        for j in range(4):
            for c in wload(it, j):
                c.wait()
        if last:
            @pl.when(i > 0)
            def _():
                for ee in range(4):
                    ucopy(4 * i - 4 + ee).wait()

        s0 = lax.rem(4 * it, W)
        for ee in range(2 if big else 4):
            e = (2 if big else 4) * i + ee
            for f0 in range(0, ff, 256):
                f = slice(f0, f0 + 256)

                def prod(w):
                    if big:
                        return (dot(xbuf[e, :, :KB], wbuf[s0 + 2 * ee, w, :, f])
                                + dot(xbuf[e, :, KB:], wbuf[s0 + 2 * ee + 1, w, :, f]))
                    return dot(xbuf[e, :, :KB], wbuf[s0 + ee, w, :, f])

                h1, h3 = prod(0), prod(1)
                if k > 0:
                    h1, h3 = acc[e, 0, :, f] + h1, acc[e, 1, :, f] + h3
                if last:
                    ubuf[ee, :, f] = (h1 * jax.nn.sigmoid(h1) * h3).astype(BF16)
                else:
                    acc[e, 0, :, f] = h1
                    acc[e, 1, :, f] = h3
        if last:
            for ee in range(4):
                ucopy(4 * i + ee).start()
        return 0

    for k in range(nk):
        gather(k)
        body = functools.partial(experts, k)
        n_it, pa, pb, pc = (small_it, 0, 2, 3) if k in (0, nk - 1) else (big_it, 1, 3, 6)

        def run(i, _):
            if k + 1 < nk:
                @pl.when(i == pa)
                def _():
                    poll_a(k + 1)
                    if k + 2 < nk:
                        own(k + 2)

                @pl.when(i == pb)
                def _():
                    poll_b(k + 1)

                @pl.when(i == pc)
                def _():
                    poll_c(k + 1)

            return body(i, 0)

        lax.fori_loop(0, n_it, run, 0)

    for e in range(n_loc - small_it, n_loc):
        ucopy(e).wait()
    for o in range(1, 8):
        mcopy(o, me).wait_send()
    for k in range(nk):
        for kind in range(KINDS):
            send(kind, k).wait_send()


def gather_up(z, meta, w1, w3):
    n_loc, d, ff = w1.shape
    t = z.shape[0]
    nk = len(CHUNKS)
    rows = n_loc * (MAIN + 4 * OVER)
    per = 8 * MAIN + 8 * OVER
    wslots = 16
    anys = pl.BlockSpec(memory_space=pl.ANY)
    vm = pl.BlockSpec(memory_space=pltpu.VMEM)
    return pl.pallas_call(
        functools.partial(up_kernel, n_loc),
        in_specs=[anys, vm, anys, anys],
        out_specs=[anys, vm],
        out_shape=[jax.ShapeDtypeStruct((n_loc, per, ff), BF16), jax.ShapeDtypeStruct((8,) + meta.shape, F32)],
        scratch_shapes=[
            pltpu.VMEM((8, t, d), BF16),
            pltpu.VMEM((8, rows, t), BF16),
            pltpu.VMEM((n_loc, per, max(CHUNKS)), BF16),
            pltpu.VMEM((n_loc, 2, per, ff), F32),
            pltpu.VMEM((wslots, 2, KB, ff), BF16),
            pltpu.VMEM((4, per, ff), BF16),
            pltpu.SemaphoreType.DMA((nk,)),
            pltpu.SemaphoreType.DMA((wslots, 2)),
            pltpu.SemaphoreType.DMA((4,)),
            pltpu.SemaphoreType.DMA((7,)),
            pltpu.SemaphoreType.DMA((7,)),
            pltpu.SemaphoreType.DMA((11, nk)),
            pltpu.SemaphoreType.DMA((11, nk)),
        ],
        compiler_params=pltpu.CompilerParams(vmem_limit_bytes=VMEM_LIMIT, collective_id=0, has_side_effects=True),
        name="gather_up",
    )(z, meta, w1, w3)


def down_kernel(n_loc, u_ref, gm_ref, w2_ref, h_ref, y_ref,
                ub, gg, ecat, wbuf, pbuf, qbuf, tbuf, drecv, xrecv, hb, usem, hsem, wsem, dss, drs, xss, xrs):
    g = Group()
    me = g.me
    t = h_ref.shape[0]
    ncb = h_ref.shape[1] // CB
    W = wbuf.shape[0]
    main = n_loc * MAIN
    rows = n_loc * (MAIN + 4 * OVER)
    hc = CB // 2

    def ucopy(i4):
        return pltpu.make_async_copy(u_ref.at[pl.ds(4 * i4, 4)], ub.at[pl.ds(4 * i4, 4)], usem.at[i4])

    for i4 in range(n_loc // 4):
        ucopy(i4).start()
    hcopy = pltpu.make_async_copy(h_ref, hb, hsem)
    hcopy.start()

    def wload(i):
        slot = lax.rem(i, W)
        e = lax.rem(i, n_loc)
        c0 = pl.multiple_of(lax.div(i, n_loc) * CB, CB)
        return pltpu.make_async_copy(w2_ref.at[e, :, pl.ds(c0, CB)], wbuf.at[slot], wsem.at[slot])

    for i in range(W - 4):
        wload(i).start()

    barrier = pltpu.get_barrier_semaphore()
    for peer in (g.right, g.left, g.other):
        pl.semaphore_signal(barrier, inc=1, device_id={"ep": peer}, device_id_type=MESH)
    pl.semaphore_wait(barrier, 3)

    base = (me * n_loc).astype(F32)

    hops = (2, 1, g.nch - 1, 0)
    places = (6, 2, 4, 0)

    def build(j, swap, _):
        p = places[j] + swap
        rank, gate = local_ranks(gm_ref[2 * lax.rem(g.chip + hops[j], g.nch) + g.core + swap * (1 - 2 * g.core)], base, n_loc)
        g_hi = gate.astype(BF16)
        r1 = gate - g_hi.astype(F32)
        g_mid = r1.astype(BF16)
        g_lo = (r1 - g_mid.astype(F32)).astype(BF16)
        for r0 in range(0, rows, 256):
            e1 = lax.broadcasted_iota(jnp.int32, (n_loc, 256), 0)
            q1 = lax.broadcasted_iota(jnp.int32, (n_loc, 256), 1) + r0
            ex = jnp.where(slot_of(q1, p, n_loc)[0] == e1, 1.0, 0.0).astype(BF16)
            want = slot_of(lax.broadcasted_iota(jnp.int32, (t, 256), 1) + r0, p, n_loc)[1].astype(F32)

            def expand(a):
                return lax.dot_general(a, ex, (((0,), (0,)), ((), ())), preferred_element_type=F32)

            keep = expand(rank) == want
            for n, part in enumerate((g_hi, g_mid, g_lo)):
                gg[p, :, n * rows + r0:n * rows + r0 + 256] = jnp.where(keep, expand(part), 0.0).astype(BF16)
        return 0

    lax.fori_loop(0, 2, functools.partial(build, 0), 0)

    def partial(p):
        e = ecat[p]
        return (dot(gg[p, :, 0:rows], e) + dot(gg[p, :, rows:2 * rows], e)) + dot(gg[p, :, 2 * rows:3 * rows], e)

    def dcopy(n, j):
        sl = lax.rem(n, 2)
        return pltpu.make_async_remote_copy(pbuf.at[sl, j], drecv.at[sl, j], dss.at[sl, j], drs.at[n, j],
                                            device_id={"ep": g.other}, device_id_type=MESH)

    def xcopy(n, kind):
        sl = lax.rem(n, 3)
        src = {0: qbuf.at[sl, 0, 0], 1: qbuf.at[sl, 0, 1], 2: qbuf.at[sl, 1, 0], 3: qbuf.at[sl, 2, 1],
               4: tbuf.at[lax.rem(n, 2), 0], 5: tbuf.at[lax.rem(n, 2), 1]}[kind]
        to = g.left if kind in (0, 3, 4) else g.right
        ssl = sl if kind < 4 else lax.rem(n, 2)
        return pltpu.make_async_remote_copy(src, xrecv.at[n, kind], xss.at[kind, ssl], xrs.at[n, kind],
                                            device_id={"ep": to}, device_id_type=MESH)

    def stage_a(n):
        sl = lax.rem(n, 2)
        sq = lax.rem(n, 3)

        def experts(i4, _):
            i = n * n_loc + 4 * i4

            @pl.when(i + W - 4 < ncb * n_loc)
            def _():
                for j in range(4):
                    wload(i + W - 4 + j).start()

            @pl.when(n == 0)
            def _():
                ucopy(i4).wait()

            for j in range(4):
                wload(i + j).wait()
            w0 = lax.rem(i, W)
            for j in range(4):
                o = dot(ub[4 * i4 + j], wbuf[w0 + j]).astype(BF16)
                r0 = pl.multiple_of((4 * i4 + j) * MAIN, MAIN)
                r1 = pl.multiple_of(main + (4 * i4 + j) * 4 * OVER, 4 * OVER)
                for s in range(8):
                    ecat[s, pl.ds(r0, MAIN), :] = o[s * MAIN:(s + 1) * MAIN]
                    b = 8 * MAIN + (s // 4) * 4 * OVER
                    ecat[s, pl.ds(r1, 4 * OVER), :] = o[b:b + 4 * OVER]
            return 0

        lax.fori_loop(0, n_loc // 4, experts, 0)

        @pl.when(n >= 3)
        def _():
            for kind in range(4):
                xcopy(n - 3, kind).wait_send()

        def finish(j):
            dcopy(n, j).wait_recv()
            qbuf[sq, j, 0] += drecv[sl, j, :, :hc]
            qbuf[sq, j, 1] += drecv[sl, j, :, hc:]
            for kind in ((0, 1), (2,), (3,), ())[j]:
                xcopy(n, kind).start()

        for j in range(4):
            if j:
                @pl.when(n == 0)
                def _():
                    lax.fori_loop(0, 2, functools.partial(build, j), 0)

            @pl.when(n >= 2)
            def _():
                dcopy(n - 2, j).wait_send()

            pbuf[sl, j] = partial(places[j] + 1)
            p = partial(places[j])
            qbuf[sq, j, 0] = p[:, :hc]
            qbuf[sq, j, 1] = p[:, hc:]
            dcopy(n, j).start()
            if j:
                finish(j - 1)
        finish(3)

    def stage_c(n):
        sq = lax.rem(n, 3)
        st = lax.rem(n, 2)

        @pl.when(n >= 2)
        def _():
            xcopy(n - 2, 4).wait_send()
            xcopy(n - 2, 5).wait_send()

        xcopy(n, 0).wait_recv()
        tbuf[st, 0] = qbuf[sq, 2, 0] + xrecv[n, 0]
        xcopy(n, 4).start()
        xcopy(n, 1).wait_recv()
        tbuf[st, 1] = qbuf[sq, 1, 1] + xrecv[n, 1]
        xcopy(n, 5).start()

    def stage_d(n):
        sq = lax.rem(n, 3)

        @pl.when(n == 0)
        def _():
            hcopy.wait()

        for kind in (2, 3, 4, 5):
            xcopy(n, kind).wait_recv()
        c0 = pl.multiple_of(n * CB, CB)
        a = (qbuf[sq, 3, 0] + xrecv[n, 2]) + xrecv[n, 4]
        b = (qbuf[sq, 3, 1] + xrecv[n, 3]) + xrecv[n, 5]
        y_ref[:, pl.ds(c0, hc)] = (hb[:, pl.ds(c0, hc)].astype(F32) + a).astype(BF16)
        y_ref[:, pl.ds(c0 + hc, hc)] = (hb[:, pl.ds(c0 + hc, hc)].astype(F32) + b).astype(BF16)

    def step(n, _):
        @pl.when(n < ncb)
        def _():
            stage_a(n)

        @pl.when(jnp.logical_and(n >= 1, n - 1 < ncb))
        def _():
            stage_c(n - 1)

        @pl.when(n >= 2)
        def _():
            stage_d(n - 2)

        return 0

    lax.fori_loop(0, ncb + 2, step, 0)

    for n in (ncb - 2, ncb - 1):
        for j in range(4):
            dcopy(n, j).wait_send()
        for kind in (4, 5):
            xcopy(n, kind).wait_send()
    for n in (ncb - 3, ncb - 2, ncb - 1):
        for kind in range(4):
            xcopy(n, kind).wait_send()


def down_reduce(u, gm, w2, h):
    n_loc, ff, d = w2.shape
    t = h.shape[0]
    ncb = d // CB
    rows = n_loc * (MAIN + 4 * OVER)
    wslots = 16
    anys = pl.BlockSpec(memory_space=pl.ANY)
    vm = pl.BlockSpec(memory_space=pltpu.VMEM)
    return pl.pallas_call(
        functools.partial(down_kernel, n_loc),
        in_specs=[anys, vm, anys, anys],
        out_specs=vm,
        out_shape=jax.ShapeDtypeStruct((t, d), BF16),
        scratch_shapes=[
            pltpu.VMEM(u.shape, BF16),
            pltpu.VMEM((8, t, 3 * rows), BF16),
            pltpu.VMEM((8, rows, CB), BF16),
            pltpu.VMEM((wslots, ff, CB), BF16),
            pltpu.VMEM((2, 4, t, CB), F32),
            pltpu.VMEM((3, 4, 2, t, CB // 2), F32),
            pltpu.VMEM((2, 2, t, CB // 2), F32),
            pltpu.VMEM((2, 4, t, CB), F32),
            pltpu.VMEM((ncb, 6, t, CB // 2), F32),
            pltpu.VMEM((t, d), BF16),
            pltpu.SemaphoreType.DMA((n_loc // 4,)),
            pltpu.SemaphoreType.DMA,
            pltpu.SemaphoreType.DMA((wslots,)),
            pltpu.SemaphoreType.DMA((2, 4)),
            pltpu.SemaphoreType.DMA((ncb, 4)),
            pltpu.SemaphoreType.DMA((6, 3)),
            pltpu.SemaphoreType.DMA((ncb, 6)),
        ],
        compiler_params=pltpu.CompilerParams(vmem_limit_bytes=VMEM_LIMIT, collective_id=1, has_side_effects=True),
        name="down_reduce",
    )(u, gm, w2, h)


def solution(mesh):
    tok = P(('dp', 'ep'))
    rep = P()
    exs = P('ep')

    def body(x, idx, gates, g1, wq, wk, wv, wo, g2, w1, w3, w2):
        n, s_len, d = x.shape
        t = n * s_len
        h, z, meta = attention(x.reshape(t, d), idx.transpose(0, 2, 1), gates.transpose(0, 2, 1), g1, g2, wq, wk, wv, wo, n)
        u, gm = gather_up(z, meta, w1, w3)
        y = down_reduce(u, gm, w2, h)
        return y.reshape(n, s_len, d)

    return jax.shard_map(body, mesh=mesh, in_specs=(tok, tok, tok, rep, rep, rep, rep, rep, rep, exs, exs, exs), out_specs=tok, check_vma=False)
```
